512 devices in a mesh: grp: 64 (over z, x_lo, core), tp: 8 (over x_hi, y).
Axes of the slice: x: 4 (x_hi: 2, x_lo: 2; x = x_hi * 2 + x_lo), y: 4, z: 16, core: 2. Of those that a mesh axis runs over, the one named last changes fastest.
Arguments:
- memory_rows: bfloat16 [65536, 4096], P('grp', 'tp'), may hold values from -24 to 24, as said below
- norm_gain: float32 [4096], replicated, may hold values from 0.25 to 1.75
- key_weight: bfloat16 [4096, 4096], P(None, 'tp'), may hold values from -0.09375 to 0.09375
- owner_table: int32 [8192], replicated, may hold values from 0 to 8191, as said below
Outputs:
- placed_keys: bfloat16 [65536, 4096], P('grp', 'tp')
The draws below stay inside these ranges and needn't reach their ends.
Inputs may be any that keep to these rules, and one draw needn't show every extreme that they name: A permutation of the 8192 block numbers. Block b of the input goes to block position owner_table[b], which lies in group owner_table[b] // 128. The 128 blocks of one group go to all 64 groups, exactly 2 blocks to each of them. `memory_rows`: rows have offsets and scales of their own, and features a common pattern.
All inputs are finite; a program needn't handle non-finite values.
Results may differ from the reference program's by a relative error of at most 0.0049.
Values may be sent and summed in bfloat16 or wider, within the bound.
No kernel may reach another device: no remote copies, remote signals or barrier semaphores. Data moves between devices by JAX's collectives and lax.ppermute only.
A program may use at most 64 MiB of HBM per device.

```python
import jax
import jax.numpy as jnp
from jax import lax

D = 4096
BLK_ROWS = 8
BLK_DEV = 128
ROWS = 65536
NB = 8192


def draw_memory_rows(key, part):
    key_off, key_scale, key_noise, key_pattern = jax.random.split(key, 4)
    offsets = jax.random.uniform(key_off, (ROWS, 1), jnp.float32, -1.5, 1.5)
    pattern = jnp.clip(jax.random.normal(key_pattern, (1, D), jnp.float32), -3.0, 3.0)
    scales = jnp.exp(jax.random.uniform(key_scale, (ROWS, 1), jnp.float32, jnp.log(0.5), jnp.log(3.0)))
    noise = jnp.clip(jax.random.normal(key_noise, (ROWS, D), jnp.float32), -4.0, 4.0)
    values = offsets + scales * (noise + 0.7 * pattern)
    return jnp.clip(values, -24.0, 24.0).astype(jnp.bfloat16)


def draw_owner_table(key, part):
    groups = NB // BLK_DEV
    per_pair = BLK_DEV // groups
    key_tau, key_offs, key_cols, key_slots = jax.random.split(key, 4)
    shuffle = jax.random.permutation(key_tau, groups).astype(jnp.int32)
    offsets = jax.random.permutation(key_offs, groups).astype(jnp.int32)
    column_keys = jax.random.split(key_cols, groups)
    column_perm = jax.vmap(lambda one_key: jax.random.permutation(one_key, BLK_DEV))(column_keys).astype(jnp.int32)
    sources = jnp.arange(groups, dtype=jnp.int32)[:, None]
    target = shuffle[(sources + offsets[column_perm % groups]) % groups]
    arrival = sources * per_pair + column_perm // groups
    slot_keys = jax.random.split(key_slots, groups)
    slot_perm = jax.vmap(lambda one_key: jax.random.permutation(one_key, BLK_DEV))(slot_keys).astype(jnp.int32)
    slots = slot_perm[target, arrival]
    return (target * BLK_DEV + slots).reshape(-1).astype(jnp.int32)


def level_of(own_key, extent, cuts, low, high):
    def one(axis_at, blocks):
        draws = jax.random.uniform(jax.random.fold_in(jax.random.fold_in(own_key, 6), axis_at), (blocks,), jnp.float32, low / len(cuts), high / len(cuts))
        return jnp.repeat(jnp.exp(draws), extent[axis_at] // blocks).reshape((-1,) + (1,) * (len(extent) - axis_at - 1))

    factor_of = one(*cuts[0])
    for cut in cuts[1:]:
        factor_of = factor_of * one(*cut)
    return factor_of


def normal_values(rng, dims, width, reach, cuts=(), kind=jnp.bfloat16):
    values = jax.random.normal(rng, dims, jnp.float32) * width
    if len(cuts) > 0:
        values = level_of(rng, dims, cuts, -0.22, 0.18) * values
    return jnp.clip(values, min=-reach, max=reach).astype(kind)


def setup_inputs(seed: int = 0) -> dict:
    arg_keys = jax.random.split(jax.random.key(seed), 5)
    memory_rows = draw_memory_rows(jax.random.fold_in(arg_keys[4], 71), 0)
    norm_gain = jnp.clip(1.0 + 0.15 * jax.random.normal(arg_keys[1], (D,), jnp.float32), 0.25, 1.75)
    key_weight = normal_values(arg_keys[2], (D, D), D ** -0.5, 0.09375, ((1, 8),))
    owner_table = draw_owner_table(jax.random.fold_in(arg_keys[4], 71), 0)
    return dict(memory_rows=memory_rows, norm_gain=norm_gain, key_weight=key_weight, owner_table=owner_table)


EPS = 1e-05

def reference(memory_rows, norm_gain, key_weight, owner_table):
    values = memory_rows.astype(jnp.float32)
    row_sum = lax.optimization_barrier(jnp.sum(values, axis=1, keepdims=True))
    row_sq = lax.optimization_barrier(jnp.sum(values * values, axis=1, keepdims=True))
    row_mean = row_sum / D
    row_var = row_sq / D - row_mean * row_mean
    normed = ((values - row_mean) * lax.rsqrt(row_var + EPS) * norm_gain[None, :]).astype(jnp.bfloat16)
    keys = jnp.dot(normed, key_weight, preferred_element_type=jnp.float32).astype(jnp.bfloat16)
    blocks = keys.reshape(NB, BLK_ROWS, D)
    placed = jnp.zeros_like(blocks).at[owner_table.astype(jnp.int32)].set(blocks)
    return placed.reshape(ROWS, D)
```

```python
import jax
import jax.numpy as jnp
import numpy as np
from jax import lax
from jax.sharding import Mesh
from jax.sharding import PartitionSpec as P

BLK_ROWS = 8
EPS = 1e-05
TORUS = ("z", "xl", "c", "xh", "y")


def torus_mesh(mesh):
    groups, parts = mesh.devices.shape
    return Mesh(mesh.devices.reshape(groups // 4, 2, 2, 2, parts // 2), TORUS)


def y_ring(step, ring):
    return [
        (core * ring + y, core * ring + (y + (step if core == 0 else -step)) % ring)
        for core in range(2)
        for y in range(ring)
    ]


def crossing():
    return [
        ((xl * 2 + c) * 2 + xh, ((1 - xl) * 2 + c) * 2 + (1 - xh))
        for xl in range(2)
        for c in range(2)
        for xh in range(2)
    ]


def gather_y(piece):
    ring = lax.axis_size("y")
    near = lax.ppermute(piece, ("c", "y"), y_ring(1, ring))
    other = lax.ppermute(piece, ("c", "y"), y_ring(-1, ring))
    far = lax.ppermute(near, ("c", "y"), y_ring(1, ring))
    return [piece, near, other, far]


def piece_owners():
    ring = lax.axis_size("y")
    y = lax.axis_index("y")
    step = 1 - 2 * lax.axis_index("c")
    return [y, (y - step) % ring, (y + step) % ring, (y + 2) % ring]


def half_weights(key_weight, norm_gain):
    xh, core = lax.axis_index("xh"), lax.axis_index("c")
    width, cols = key_weight.shape
    half, quarter, depth = width // 2, width // 4, width // 8
    sent = lax.dynamic_slice(
        key_weight, ((1 - xh) * half + core * quarter, 0), (quarter, cols)
    )
    mine = lax.ppermute(sent, ("xl", "c", "xh"), crossing())
    twin = lax.ppermute(mine, "c", [(0, 1), (1, 0)])
    swapped = jnp.concatenate([mine, twin], axis=0)
    own_parts, other_parts, gain_parts = [], [], []
    for owner in piece_owners():
        start = xh * half + owner * depth
        own_parts.append(lax.dynamic_slice(key_weight, (start, 0), (depth, cols)))
        place = ((owner // 2) ^ core) * 2 + owner % 2
        other_parts.append(lax.dynamic_slice(swapped, (place * depth, 0), (depth, cols)))
        gain_parts.append(lax.dynamic_slice(norm_gain, (start,), (depth,)))
    own = jnp.concatenate(own_parts, axis=0)
    other = jnp.concatenate(other_parts, axis=0)
    first = xh == 0
    weights = jnp.concatenate(
        [jnp.where(first, own, other), jnp.where(first, other, own)], axis=1
    )
    gain = jnp.concatenate(gain_parts)
    gain_sums = jnp.sum(gain[:, None] * weights.astype(jnp.float32), axis=0)
    return weights, gain, gain_sums


def partial_keys(pieces, weights, gain, gain_sums):
    values = jnp.concatenate(pieces, axis=1).astype(jnp.float32)
    half = values.shape[1]
    sums = jnp.sum(values, axis=1)
    squares = jnp.sum(values * values, axis=1)
    here = jnp.stack([sums, squares])
    there = lax.ppermute(here, "xh", [(0, 1), (1, 0)])
    center = sums / half
    scaled = ((values - center[:, None]) * gain[None, :]).astype(jnp.bfloat16)
    product = jnp.dot(scaled, weights, preferred_element_type=jnp.float32)
    both = here + there
    mean = both[0] / (2 * half)
    var = both[1] / (2 * half) - mean * mean
    shifted = product + (center - mean)[:, None] * gain_sums[None, :]
    return (shifted * lax.rsqrt(var + EPS)[:, None]).astype(jnp.bfloat16)


def exchange_x(partial):
    targets, rows, width = partial.shape
    cols = width // 2
    outgoing = partial.reshape(targets, rows, 2, cols).transpose(0, 2, 1, 3)
    outgoing = outgoing.reshape(targets * 2, rows, cols)
    incoming = lax.all_to_all(outgoing, ("xl", "c", "xh"), 0, 0, tiled=True)
    incoming = incoming.reshape(targets, 2, rows, cols).astype(jnp.float32)
    return (incoming[:, 0] + incoming[:, 1]).astype(jnp.bfloat16)


def arrival_slots(owner_table, group, groups, blocks):
    table = owner_table.reshape(groups, blocks)
    ids = jnp.arange(blocks, dtype=jnp.int32)[None, :]
    here = table // blocks == group
    first = jnp.min(jnp.where(here, ids, blocks), axis=1, keepdims=True)
    slots = table % blocks
    slot_a = jnp.sum(jnp.where(ids == first, slots, 0), axis=1)
    slot_b = jnp.sum(jnp.where(here & (ids != first), slots, 0), axis=1)
    return slot_a, slot_b


def on_device(memory_rows, norm_gain, key_weight, owner_table):
    depth_z = lax.axis_size("z")
    groups = 4 * depth_z
    group = (
        lax.axis_index("z") * 4 + lax.axis_index("xl") * 2 + lax.axis_index("c")
    )
    rows, cols = memory_rows.shape
    blocks = rows // BLK_ROWS
    half_rows = rows // 2
    owned = lax.dynamic_slice_in_dim(owner_table, group * blocks, blocks)
    target = owned // blocks
    ids = jnp.arange(blocks, dtype=jnp.int32)
    earlier = (target[None, :] == target[:, None]) & (ids[None, :] < ids[:, None])
    first = jnp.sum(earlier.astype(jnp.int32), axis=1) == 0
    slot = jnp.where(first, target, groups + (target % 4) * depth_z + target // 4)
    sender = (slot[None, :] == ids[:, None]).astype(jnp.bfloat16)
    flattened = memory_rows.reshape(blocks, BLK_ROWS * cols)
    packed = jnp.dot(sender, flattened, preferred_element_type=jnp.float32)
    packed = packed.astype(jnp.bfloat16).reshape(2, half_rows, cols)

    pieces_g = gather_y(packed[1])
    rows_p = lax.all_to_all(
        packed[0].reshape(depth_z, half_rows // depth_z, cols), "z", 0, 0, tiled=True
    )
    weights, gain, gain_sums = half_weights(key_weight, norm_gain)

    partial_g = partial_keys(pieces_g, weights, gain, gain_sums)
    keys_g = exchange_x(partial_g.reshape(4, half_rows // 4, 2 * cols))
    keys_g = keys_g.reshape(4, depth_z, BLK_ROWS, cols).transpose(1, 0, 2, 3)
    keys_g = lax.all_to_all(
        keys_g.reshape(depth_z, 4 * BLK_ROWS, cols), "z", 0, 0, tiled=True
    )

    rows_p = rows_p.reshape(depth_z, 4, BLK_ROWS, cols).transpose(1, 0, 2, 3)
    pieces_p = gather_y(rows_p.reshape(half_rows, cols))
    partial_p = partial_keys(pieces_p, weights, gain, gain_sums)
    keys_p = exchange_x(partial_p.reshape(4, half_rows // 4, 2 * cols))

    slot_a, slot_b = arrival_slots(owner_table, group, groups, blocks)
    slot_a = slot_a.reshape(depth_z, 4).T.reshape(groups)
    slots = jnp.concatenate([slot_a, slot_b])
    picker = (slots[None, :] == ids[:, None]).astype(jnp.bfloat16)
    arrived = jnp.concatenate(
        [
            keys_p.reshape(groups, BLK_ROWS * cols),
            keys_g.reshape(groups, BLK_ROWS * cols),
        ]
    )
    placed = jnp.dot(picker, arrived, preferred_element_type=jnp.float32)
    return placed.astype(jnp.bfloat16).reshape(rows, cols)


def solution(mesh):
    groups, parts = ("z", "xl", "c"), ("xh", "y")
    in_specs = (P(groups, parts), P(), P(None, parts), P())
    return jax.shard_map(
        on_device,
        mesh=torus_mesh(mesh),
        in_specs=in_specs,
        out_specs=P(groups, parts),
        check_vma=False,
    )
```

```python
import functools

import jax
import jax.numpy as jnp
from jax import lax
from jax.experimental import pallas as pl
from jax.experimental.pallas import tpu as pltpu
from jax.sharding import Mesh
from jax.sharding import PartitionSpec as P

BLK = 8
EPS = 1e-05
TORUS = ("z", "xl", "c", "xh", "y")
SUBCUBE = ("xl", "c", "xh")
VMEM = pl.BlockSpec(memory_space=pltpu.VMEM)
SMEM = pl.BlockSpec(memory_space=pltpu.SMEM)
F32, BF16 = jnp.float32, jnp.bfloat16


def torus_mesh(mesh):
    groups, parts = mesh.devices.shape
    return Mesh(mesh.devices.reshape(groups // 4, 2, 2, 2, parts // 2), TORUS)


def y_ring(step, ring):
    return [
        (core * ring + y, core * ring + (y + (step if core == 0 else -step)) % ring)
        for core in range(2)
        for y in range(ring)
    ]


def crossing():
    return [
        ((xl * 2 + c) * 2 + xh, ((1 - xl) * 2 + c) * 2 + (1 - xh))
        for xl in range(2)
        for c in range(2)
        for xh in range(2)
    ]


def gather_y(piece):
    ring = lax.axis_size("y")
    near = lax.ppermute(piece, ("c", "y"), y_ring(1, ring))
    other = lax.ppermute(piece, ("c", "y"), y_ring(-1, ring))
    far = lax.ppermute(near, ("c", "y"), y_ring(1, ring))
    return [piece, near, other, far]


def pack_kernel(groups, owned, rows, first, second, count):
    blocks = rows.shape[0]
    shift = blocks.bit_length() - 1

    def clear(i, carry):
        count[i] = 0
        return carry

    def place(b, carry):
        target = owned[b] >> shift
        seen = count[target]
        count[target] = seen + 1

        @pl.when(seen == 0)
        def _():
            first[target] = rows[b]

        @pl.when(seen != 0)
        def _():
            second[target] = rows[b]

        return carry

    lax.fori_loop(0, groups, clear, 0, unroll=8)
    lax.fori_loop(0, blocks, place, 0, unroll=4)


def pack(memory_rows, owned, groups):
    rows, cols = memory_rows.shape
    blocks = rows // BLK
    out = jax.ShapeDtypeStruct((groups, BLK, cols), BF16)
    return pl.pallas_call(
        functools.partial(pack_kernel, groups),
        out_shape=(out, out),
        in_specs=[SMEM, VMEM],
        out_specs=(VMEM, VMEM),
        scratch_shapes=[pltpu.SMEM((groups,), jnp.int32)],
        cost_estimate=pl.CostEstimate(flops=1 << 20, bytes_accessed=4 * rows * cols, transcendentals=0),
        name="pack",
    )(owned, memory_rows.reshape(blocks, BLK, cols))


def two_parts(value):
    high = value.astype(BF16).astype(F32)
    return high, value - high


def key_kernel(where, p0, p1, p2, p3, gain, w_own, w_mine, w_twin, kept, table, sent, scaled, acc):
    step = pl.program_id(0)
    parts = (p0, p1, p2, p3)
    rows, width = p0.shape
    half = width * 4
    tile = 128
    tiles = rows // BLK

    @pl.when(step == 0)
    def _():
        sent[tiles] = jnp.zeros(sent.shape[1:], BF16)
        for q in range(rows // tile):
            here = pl.ds(q * tile, tile)
            total = jnp.zeros((tile, 1), F32)
            square = jnp.zeros((tile, 1), F32)
            for part in parts:
                v = part[here, :].astype(F32)
                total += jnp.sum(v, axis=1, keepdims=True)
                square += jnp.sum(v * v, axis=1, keepdims=True)
            mean = total / half
            center, rest = two_parts(mean)
            high, low = two_parts(square / half - mean * mean)
            for j, part in enumerate(parts):
                v = part[here, :].astype(F32)
                scaled[j, here, :] = ((v - center) * gain[j]).astype(BF16)
            lane = lax.broadcasted_iota(jnp.int32, (tile, 128), 1)
            stats = jnp.where(lane == 0, center, 0.0)
            stats = jnp.where(lane == 1, rest, stats)
            stats = jnp.where(lane == 2, high, stats)
            stats = jnp.where(lane == 3, low, stats)
            table[here, :] = stats
            sent[tiles, :, q * 128 : (q + 1) * 128] = jnp.transpose(stats)[0:BLK, :].astype(BF16)

    left = scaled[step]
    from_mine = where[4 + step] < 2
    own = jnp.dot(left, w_own[...], preferred_element_type=F32)

    @pl.when(step == 0)
    def _():
        kept[...] = own
        acc[...] = jnp.zeros_like(own)

    @pl.when(step != 0)
    def _():
        kept[...] += own

    @pl.when(from_mine)
    def _():
        acc[...] += jnp.dot(left, w_mine[...], preferred_element_type=F32)

    @pl.when(jnp.logical_not(from_mine))
    def _():
        acc[...] += jnp.dot(left, w_twin[...], preferred_element_type=F32)

    @pl.when(step == 3)
    def _():
        sent[0:tiles] = acc[...].reshape(tiles, BLK, acc.shape[1]).astype(BF16)


def project(pieces, where, gain, key_weight, mine, twin):
    rows, width = pieces[0].shape
    tiles = rows // BLK
    cols = key_weight.shape[1]
    whole = pl.BlockSpec((rows, width), lambda j, s: (0, 0))
    return pl.pallas_call(
        key_kernel,
        out_shape=(
            jax.ShapeDtypeStruct((rows, cols), F32),
            jax.ShapeDtypeStruct((rows, 128), F32),
            jax.ShapeDtypeStruct((tiles + 1, BLK, cols), BF16),
        ),
        grid_spec=pltpu.PrefetchScalarGridSpec(
            num_scalar_prefetch=1,
            grid=(4,),
            in_specs=[whole] * 4
            + [
                pl.BlockSpec((4, 1, width), lambda j, s: (0, 0, 0)),
                pl.BlockSpec((width, cols), lambda j, s: (s[j], 0)),
                pl.BlockSpec((width, cols), lambda j, s: (s[4 + j] & 1, 0)),
                pl.BlockSpec((width, cols), lambda j, s: (s[4 + j] & 1, 0)),
            ],
            out_specs=(
                pl.BlockSpec((rows, cols), lambda j, s: (0, 0)),
                pl.BlockSpec((rows, 128), lambda j, s: (0, 0)),
                pl.BlockSpec((tiles + 1, BLK, cols), lambda j, s: (0, 0, 0)),
            ),
            scratch_shapes=[
                pltpu.VMEM((4, rows, width), BF16),
                pltpu.VMEM((rows, cols), F32),
            ],
        ),
        cost_estimate=pl.CostEstimate(
            flops=2 * rows * width * 4 * cols * 2, bytes_accessed=8 << 20, transcendentals=0
        ),
    )(where, *pieces, gain, key_weight, mine, twin)


def whole_keys(kept, table, came, gain_sums, q):
    tiles = came.shape[0] - 1
    cols = came.shape[2]
    here = pl.ds(q * 128, 128)
    per = 128 // BLK
    value_b = came[q * per : (q + 1) * per].astype(F32).reshape(128, cols)
    stats = came[tiles, :, q * 128 : (q + 1) * 128].astype(F32)
    stats = jnp.concatenate([stats, jnp.zeros((128 - BLK, 128), F32)], axis=0)
    stats_b = jnp.transpose(stats)
    stats_a = table[here, :]
    center_a, center_b = stats_a[:, 0:1], stats_b[:, 0:1]
    mean_a, mean_b = center_a + stats_a[:, 1:2], center_b + stats_b[:, 1:2]
    var_a, var_b = stats_a[:, 2:3] + stats_a[:, 3:4], stats_b[:, 2:3] + stats_b[:, 3:4]
    mean = 0.5 * (mean_a + mean_b)
    gap = 0.5 * (mean_a - mean_b)
    scale = lax.rsqrt(0.5 * (var_a + var_b) + gap * gap + EPS)
    shift = (center_a - mean) * gain_sums[0:1, :] + (center_b - mean) * gain_sums[1:2, :]
    keys = (kept[here, :] + value_b + shift) * scale
    return keys.reshape(per, BLK, cols).astype(BF16)


def sum_kernel(kept, table, came, gain_sums, out):
    per = 128 // BLK
    for q in range(kept.shape[0] // 128):
        out[q * per : (q + 1) * per] = whole_keys(kept, table, came, gain_sums, q)


def sum_partials(kept, table, came, gain_sums):
    tiles, _, cols = came.shape
    return pl.pallas_call(
        sum_kernel,
        out_shape=jax.ShapeDtypeStruct((tiles - 1, BLK, cols), BF16),
        in_specs=[VMEM] * 4,
        out_specs=VMEM,
        cost_estimate=pl.CostEstimate(flops=1 << 22, bytes_accessed=4 << 20, transcendentals=0),
        name="sum_g",
    )(kept, table, came, gain_sums)


def place_kernel(slots, kept, table, came, gain_sums, others, out):
    groups = others.shape[0]
    per = 128 // BLK
    for q in range(kept.shape[0] // 128):
        keys = whole_keys(kept, table, came, gain_sums, q)
        for i in range(per):
            out[slots[q * per + i]] = keys[i]

    def put(i, carry):
        out[slots[groups + i]] = others[i]
        return carry

    lax.fori_loop(0, groups, put, 0, unroll=8)


def place(slots, kept, table, came, gain_sums, others):
    _, _, cols = came.shape
    blocks = slots.shape[0]
    return pl.pallas_call(
        place_kernel,
        out_shape=jax.ShapeDtypeStruct((blocks, BLK, cols), BF16),
        in_specs=[SMEM] + [VMEM] * 5,
        out_specs=VMEM,
        cost_estimate=pl.CostEstimate(flops=1 << 22, bytes_accessed=4 << 20, transcendentals=0),
        name="place",
    )(slots, kept, table, came, gain_sums, others)


def arrival_slots(owner_table, group, groups, blocks):
    table = owner_table.reshape(groups, blocks)
    ids = jnp.arange(blocks, dtype=jnp.int32)[None, :]
    here = table // blocks == group
    first = jnp.min(jnp.where(here, ids, blocks), axis=1, keepdims=True)
    slots = table % blocks
    slot_a = jnp.sum(jnp.where(ids == first, slots, 0), axis=1)
    slot_b = jnp.sum(jnp.where(here & (ids != first), slots, 0), axis=1)
    return jnp.concatenate([slot_a, slot_b])


def steps(memory_rows, norm_gain, key_weight, owner_table):
    depth_z = lax.axis_size("z")
    ring = lax.axis_size("y")
    groups = 4 * depth_z
    xh, core, y = lax.axis_index("xh"), lax.axis_index("c"), lax.axis_index("y")
    group = lax.axis_index("z") * 4 + lax.axis_index("xl") * 2 + core
    rows, cols = memory_rows.shape
    blocks, half_rows = rows // BLK, rows // 2
    width, outs = key_weight.shape

    sent = lax.dynamic_slice(
        key_weight,
        ((1 - xh) * (width // 2) + core * (width // 4), 0),
        (width // 4, outs),
    )
    mine = lax.ppermute(sent, SUBCUBE, crossing())
    twin = lax.ppermute(mine, "c", [(0, 1), (1, 0)])

    owned = lax.dynamic_slice_in_dim(owner_table, group * blocks, blocks)
    packed_p, packed_g = pack(memory_rows, owned, groups)
    pieces_g = gather_y(packed_g.reshape(half_rows, cols))
    rows_p = lax.all_to_all(packed_p, ("z", "xl", "c"), 0, 0, tiled=True)

    step = 1 - 2 * core
    owners = jnp.stack([y, (y - step) % ring, (y + step) % ring, (y + 2) % ring])
    places = ((owners // 2) ^ core) * 2 + owners % 2
    where = jnp.concatenate([xh * 4 + owners, places, xh[None]]).astype(jnp.int32)
    gain = norm_gain.reshape(8, 1, cols)[xh * 4 + owners]
    gain_sums = jnp.sum(
        (norm_gain[:, None] * key_weight.astype(F32)).reshape(2, width // 2, outs), axis=1
    )
    gain_sums = jnp.where(xh == 0, gain_sums, gain_sums[::-1])
    slots = arrival_slots(owner_table, group, groups, blocks)

    pair = [(0, 1), (1, 0)]
    kept_g, table_g, sent_g = project(pieces_g, where, gain, key_weight, mine, twin)
    came_g = lax.ppermute(sent_g, "xh", pair)
    keys_g = sum_partials(kept_g, table_g, came_g, gain_sums)
    keys_g = lax.all_to_all(keys_g, ("z", "xl", "c"), 0, 0, tiled=True)

    pieces_p = gather_y(rows_p.reshape(half_rows, cols))
    kept_p, table_p, sent_p = project(pieces_p, where, gain, key_weight, mine, twin)
    came_p = lax.ppermute(sent_p, "xh", pair)
    placed = place(slots, kept_p, table_p, came_p, gain_sums, keys_g)
    return placed.reshape(rows, outs)


def solution(mesh):
    groups, parts = ("z", "xl", "c"), ("xh", "y")
    torus = torus_mesh(mesh)
    return jax.shard_map(
        steps,
        mesh=torus,
        in_specs=(P(groups, parts), P(), P(None, parts), P()),
        out_specs=P(groups, parts),
        check_vma=False,
    )
```

```python
import functools

import jax
import jax.numpy as jnp
from jax import lax
from jax.experimental import pallas as pl
from jax.experimental.pallas import tpu as pltpu
from jax.sharding import Mesh
from jax.sharding import PartitionSpec as P

BLK = 8
EPS = 1e-05
TORUS = ("z", "xl", "c", "xh", "y")
SUBCUBE = ("xl", "c", "xh")
SPREAD = ("c", "z", "xl")
VMEM = pl.BlockSpec(memory_space=pltpu.VMEM)
SMEM = pl.BlockSpec(memory_space=pltpu.SMEM)
F32, BF16 = jnp.float32, jnp.bfloat16


def torus_mesh(mesh):
    groups, parts = mesh.devices.shape
    return Mesh(mesh.devices.reshape(groups // 4, 2, 2, 2, parts // 2), TORUS)


def crossing():
    return [
        ((xl * 2 + c) * 2 + xh, ((1 - xl) * 2 + c) * 2 + (1 - xh))
        for xl in range(2)
        for c in range(2)
        for xh in range(2)
    ]


def gather_y(piece):
    ring = lax.axis_size("y")

    def send(step):
        return lax.ppermute(piece, "y", [(y, (y + step) % ring) for y in range(ring)])

    far = send(2)
    near = send(1)
    other = send(-1)
    return [piece, far, near, other]


def pack_kernel(groups, table, rows, weights, first, second, leaving, count, staged, sems):
    blocks = rows.shape[0]
    shift = blocks.bit_length() - 1
    quarter = staged.shape[0]
    xh, core = lax.axis_index("xh"), lax.axis_index("c")
    group = lax.axis_index("z") * 4 + lax.axis_index("xl") * 2 + core
    base = group * blocks
    start = pl.multiple_of(((1 - xh) * 2 + core) * quarter, quarter)
    load = pltpu.make_async_copy(weights.at[pl.ds(start, quarter), :], staged, sems.at[0])
    store = pltpu.make_async_copy(staged, leaving, sems.at[1])
    load.start()

    def clear(i, carry):
        count[i] = 0
        return carry

    def put(b, carry):
        target = table[base + b] >> shift
        seen = count[target]
        count[target] = seen + 1
        spot = (target & 1) * (groups // 2) + (target >> 1)

        @pl.when(seen == 0)
        def _():
            first[spot] = rows[b]

        @pl.when(seen != 0)
        def _():
            second[spot] = rows[b]

        return carry

    lax.fori_loop(0, groups, clear, 0, unroll=8)
    lax.fori_loop(0, blocks // 2, put, 0, unroll=4)
    load.wait()
    store.start()
    lax.fori_loop(blocks // 2, blocks, put, 0, unroll=4)
    store.wait()


def grant(mib):
    return pltpu.CompilerParams(vmem_limit_bytes=mib << 20)


def cost():
    return pl.CostEstimate(flops=1 << 34, bytes_accessed=0, transcendentals=0)


ANY = pl.BlockSpec(memory_space=pl.ANY)


def pack(memory_rows, owner_table, key_weight, groups):
    rows, cols = memory_rows.shape
    width, outs = key_weight.shape
    blocks = rows // BLK
    out = jax.ShapeDtypeStruct((groups, BLK, cols), BF16)
    return pl.pallas_call(
        functools.partial(pack_kernel, groups),
        out_shape=(out, out, jax.ShapeDtypeStruct((width // 4, outs), BF16)),
        in_specs=[SMEM, VMEM, ANY],
        out_specs=(VMEM, VMEM, ANY),
        scratch_shapes=[
            pltpu.SMEM((groups,), jnp.int32),
            pltpu.VMEM((width // 4, outs), BF16),
            pltpu.SemaphoreType.DMA((2,)),
        ],
        cost_estimate=cost(),
        name="pack",
    )(owner_table, memory_rows.reshape(blocks, BLK, cols), key_weight)


def owners():
    y, ring = lax.axis_index("y"), lax.axis_size("y")
    return [y, lax.rem(y + 2, ring), lax.rem(y + ring - 1, ring), lax.rem(y + 1, ring)]


def gain_rows(gain):
    high = gain.astype(BF16).astype(F32)
    middle = (gain - high).astype(BF16).astype(F32)
    zeros = jnp.zeros((BLK - 3, gain.shape[1]), F32)
    return jnp.concatenate([high, middle, gain - high - middle, zeros], axis=0).astype(BF16)


def two_parts(value):
    high = value.astype(BF16).astype(F32)
    return high, value - high


def fold(value):
    lanes = [value[:, i : i + 128] for i in range(0, value.shape[1], 128)]
    return functools.reduce(jnp.add, lanes)


def sent_kernel(p0, p1, p2, p3, gains, w_mine, w_twin, table, sent, raw, scaled, held, sums, acc, sems):
    rows, width = p0.shape
    half = width * 4
    tile = 128
    tiles = rows // BLK
    xh, core = lax.axis_index("xh"), lax.axis_index("c")
    gain = [gains[xh * 4 + owner] for owner in owners()]
    piece_copies = [
        pltpu.make_async_copy(part, raw.at[j], sems.at[j]) for j, part in enumerate((p0, p1, p2, p3))
    ]
    deep = held.shape[0] // 2
    mine_copy = pltpu.make_async_copy(w_mine, held.at[0:deep], sems.at[4])
    twin_copy = pltpu.make_async_copy(w_twin, held.at[deep : 2 * deep], sems.at[5])
    for copy in piece_copies:
        copy.start()
    mine_copy.start()
    twin_copy.start()

    sent[tiles] = jnp.zeros(sent.shape[1:], BF16)
    for j in range(4):
        piece_copies[j].wait()
        for q in range(rows // tile):
            here = pl.ds(q * tile, tile)
            v = raw[j, here, :].astype(F32)
            total, square = fold(v), fold(v * v)
            if j == 0:
                sums[0, here], sums[1, here] = total, square
            else:
                sums[0, here] += total
                sums[1, here] += square
    for q in range(rows // tile):
        here = pl.ds(q * tile, tile)
        mean = jnp.sum(sums[0, here], axis=1, keepdims=True) / half
        square = jnp.sum(sums[1, here], axis=1, keepdims=True) / half
        center, rest = two_parts(mean)
        high, low = two_parts(square - mean * mean)
        for j in range(4):
            v = raw[j, here, :].astype(F32)
            scaled[j, here, :] = ((v - center) * gain[j]).astype(BF16)
        lane = lax.broadcasted_iota(jnp.int32, (tile, 128), 1)
        stats = jnp.where(lane == 0, center, 0.0)
        stats = jnp.where(lane == 1, rest, stats)
        stats = jnp.where(lane == 2, high, stats)
        stats = jnp.where(lane == 3, low, stats)
        table[here, :] = stats
        sent[tiles, :, q * 128 : (q + 1) * 128] = jnp.transpose(stats)[0:BLK, :].astype(BF16)

    mine_copy.wait()
    twin_copy.wait()
    gain_sum = jnp.zeros((BLK, acc.shape[1]), F32)
    for j, owner in enumerate(owners()):
        slot = ((owner >> 1) ^ core) * 2 + (owner & 1)
        block = held[pl.ds(pl.multiple_of(slot * width, width), width), :]
        gain_sum += jnp.dot(gain_rows(gain[j]), block, preferred_element_type=F32)
        part = jnp.dot(scaled[j], block, preferred_element_type=F32)
        if j == 0:
            acc[...] = part
        elif j < 3:
            acc[...] += part
        else:
            sent[0:tiles] = (acc[...] + part).reshape(tiles, BLK, part.shape[1]).astype(BF16)
    total = jnp.sum(gain_sum, axis=0, keepdims=True)
    high, rest = two_parts(total)
    middle, low = two_parts(rest)
    row = lax.broadcasted_iota(jnp.int32, (BLK, width), 0)
    extra = sent[tiles].astype(F32)
    for place, value in ((4, high), (5, middle), (6, low)):
        extra = jnp.where(row == place, value, extra)
    sent[tiles] = extra.astype(BF16)


def project_sent(pieces, gains, mine, twin):
    rows, width = pieces[0].shape
    tiles = rows // BLK
    deep, cols = mine.shape
    return pl.pallas_call(
        sent_kernel,
        out_shape=(
            jax.ShapeDtypeStruct((rows, 128), F32),
            jax.ShapeDtypeStruct((tiles + 1, BLK, cols), BF16),
        ),
        in_specs=[ANY] * 4 + [VMEM] + [ANY] * 2,
        out_specs=(VMEM, VMEM),
        scratch_shapes=[
            pltpu.VMEM((4, rows, width), BF16),
            pltpu.VMEM((4, rows, width), BF16),
            pltpu.VMEM((2 * deep, cols), BF16),
            pltpu.VMEM((2, rows, 128), F32),
            pltpu.VMEM((rows, cols), F32),
            pltpu.SemaphoreType.DMA((6,)),
        ],
        compiler_params=grant(12),
        cost_estimate=cost(),
    )(*pieces, gains, mine, twin)


def kept_kernel(half_id, p0, p1, p2, p3, table, gains, w_own, kept, gain_sums):
    width = p0.shape[1]
    center = table[:, 0:1]
    xh = lax.axis_index("xh")
    total = jnp.zeros((BLK, kept.shape[1]), F32)
    for j, (part, owner) in enumerate(zip((p0, p1, p2, p3), owners())):
        gain = gains[xh * 4 + owner]
        block = w_own[pl.ds(pl.multiple_of(owner * width, width), width), :]
        scaled = ((part[...].astype(F32) - center) * gain).astype(BF16)
        total += jnp.dot(gain_rows(gain), block, preferred_element_type=F32)
        product = jnp.dot(scaled, block, preferred_element_type=F32)
        if j == 0:
            kept[...] = product
        else:
            kept[...] += product
    gain_sums[...] = jnp.broadcast_to(jnp.sum(total, axis=0, keepdims=True), total.shape)


def project_kept(pieces, table, half_id, gains, key_weight):
    rows, width = pieces[0].shape
    half, cols = key_weight.shape[0] // 2, key_weight.shape[1]
    whole = pl.BlockSpec((rows, width), lambda i, s: (0, 0))
    return pl.pallas_call(
        kept_kernel,
        out_shape=(
            jax.ShapeDtypeStruct((rows, cols), F32),
            jax.ShapeDtypeStruct((BLK, cols), F32),
        ),
        grid_spec=pltpu.PrefetchScalarGridSpec(
            num_scalar_prefetch=1,
            grid=(1,),
            in_specs=[whole] * 4
            + [
                pl.BlockSpec((rows, 128), lambda i, s: (0, 0)),
                pl.BlockSpec(gains.shape, lambda i, s: (0, 0, 0)),
                pl.BlockSpec((half, cols), lambda i, s: (s[0], 0)),
            ],
            out_specs=(
                pl.BlockSpec((rows, cols), lambda i, s: (0, 0)),
                pl.BlockSpec((BLK, cols), lambda i, s: (0, 0)),
            ),
        ),
        compiler_params=grant(16),
        cost_estimate=cost(),
    )(half_id, *pieces, table, gains, key_weight)


def whole_keys(kept, table, came, gain_sums, q):
    tiles = came.shape[0] - 1
    cols = came.shape[2]
    here = pl.ds(q * 128, 128)
    per = 128 // BLK
    value_b = came[q * per : (q + 1) * per].astype(F32).reshape(128, cols)
    stats = came[tiles, :, q * 128 : (q + 1) * 128].astype(F32)
    stats = jnp.concatenate([stats, jnp.zeros((128 - BLK, 128), F32)], axis=0)
    stats_b = jnp.transpose(stats)
    stats_a = table[here, :]
    center_a, center_b = stats_a[:, 0:1], stats_b[:, 0:1]
    mean_a, mean_b = center_a + stats_a[:, 1:2], center_b + stats_b[:, 1:2]
    var_a, var_b = stats_a[:, 2:3] + stats_a[:, 3:4], stats_b[:, 2:3] + stats_b[:, 3:4]
    mean = 0.5 * (mean_a + mean_b)
    gap = 0.5 * (mean_a - mean_b)
    scale = lax.rsqrt(0.5 * (var_a + var_b) + gap * gap + EPS)
    sums_b = jnp.sum(came[tiles, 4:7, :].astype(F32), axis=0, keepdims=True)
    shift = (center_a - mean) * gain_sums[0:1, :] + (center_b - mean) * sums_b
    keys = (kept[here, :] + value_b + shift) * scale
    return keys.reshape(per, BLK, cols).astype(BF16)


def sum_kernel(kept, table, came, gain_sums, out):
    per = 128 // BLK
    for q in range(kept.shape[0] // 128):
        out[q * per : (q + 1) * per] = whole_keys(kept, table, came, gain_sums, q)


def sum_partials(kept, table, came, gain_sums):
    tiles, _, cols = came.shape
    return pl.pallas_call(
        sum_kernel,
        out_shape=jax.ShapeDtypeStruct((tiles - 1, BLK, cols), BF16),
        in_specs=[VMEM] * 4,
        out_specs=VMEM,
        compiler_params=grant(16),
        cost_estimate=cost(),
        name="sum_g",
    )(kept, table, came, gain_sums)


def place_kernel(slots, kept, table, came, gain_sums, others, out):
    groups = others.shape[0]
    per = 128 // BLK
    for q in range(kept.shape[0] // 128):
        keys = whole_keys(kept, table, came, gain_sums, q)
        for i in range(per):
            out[slots[q * per + i]] = keys[i]

    def put(i, carry):
        out[slots[groups + i]] = others[i]
        return carry

    lax.fori_loop(0, groups, put, 0, unroll=8)


def place(slots, kept, table, came, gain_sums, others):
    _, _, cols = came.shape
    blocks = slots.shape[0]
    return pl.pallas_call(
        place_kernel,
        out_shape=jax.ShapeDtypeStruct((blocks, BLK, cols), BF16),
        in_specs=[SMEM] + [VMEM] * 5,
        out_specs=VMEM,
        compiler_params=grant(16),
        cost_estimate=cost(),
        name="place",
    )(slots, kept, table, came, gain_sums, others)


def arrival_slots(owner_table, group, groups, blocks):
    table = owner_table.reshape(groups, blocks)
    ids = jnp.arange(blocks, dtype=jnp.int32)[None, :]
    here = table // blocks == group
    first = jnp.min(jnp.where(here, ids, blocks), axis=1, keepdims=True)
    slots = table % blocks
    slot_a = jnp.sum(jnp.where(ids == first, slots, 0), axis=1)
    slot_b = jnp.sum(jnp.where(here & (ids != first), slots, 0), axis=1)
    by_source = [
        slot.reshape(groups // 2, 2).T.reshape(groups) for slot in (slot_a, slot_b)
    ]
    return jnp.concatenate(by_source)


def steps(memory_rows, norm_gain, key_weight, owner_table):
    depth_z = lax.axis_size("z")
    groups = 4 * depth_z
    xh, core = lax.axis_index("xh"), lax.axis_index("c")
    group = lax.axis_index("z") * 4 + lax.axis_index("xl") * 2 + core
    rows, cols = memory_rows.shape
    blocks, half_rows = rows // BLK, rows // 2
    width, outs = key_weight.shape

    packed_p, packed_g, leaving = pack(memory_rows, owner_table, key_weight, groups)
    mine = lax.ppermute(leaving, SUBCUBE, crossing())
    twin = lax.ppermute(mine, "c", [(0, 1), (1, 0)])
    pieces_g = gather_y(packed_g.reshape(half_rows, cols))
    rows_p = lax.all_to_all(packed_p, SPREAD, 0, 0, tiled=True)

    gains = norm_gain.reshape(width // cols, 1, cols)
    half_id = xh.reshape(1).astype(jnp.int32)
    slots = arrival_slots(owner_table, group, groups, blocks)

    pair = [(0, 1), (1, 0)]
    table_g, sent_g = project_sent(pieces_g, gains, mine, twin)
    came_g = lax.ppermute(sent_g, "xh", pair)
    kept_g, gain_sums_g = project_kept(pieces_g, table_g, half_id, gains, key_weight)
    keys_g = sum_partials(kept_g, table_g, came_g, gain_sums_g)
    keys_g = lax.all_to_all(keys_g, SPREAD, 0, 0, tiled=True)

    pieces_p = gather_y(rows_p.reshape(half_rows, cols))
    table_p, sent_p = project_sent(pieces_p, gains, mine, twin)
    came_p = lax.ppermute(sent_p, "xh", pair)
    kept_p, gain_sums_p = project_kept(pieces_p, table_p, half_id, gains, key_weight)
    placed = place(slots, kept_p, table_p, came_p, gain_sums_p, keys_g)
    return placed.reshape(rows, outs)


def solution(mesh):
    groups, parts = ("z", "xl", "c"), ("xh", "y")
    torus = torus_mesh(mesh)
    return jax.shard_map(
        steps,
        mesh=torus,
        in_specs=(P(groups, parts), P(), P(None, parts), P()),
        out_specs=P(groups, parts),
        check_vma=False,
    )
```

```python
import functools

import jax
import jax.numpy as jnp
from jax import lax
from jax.experimental import pallas as pl
from jax.experimental.pallas import tpu as pltpu
from jax.sharding import Mesh
from jax.sharding import PartitionSpec as P

BLK = 8
EPS = 1e-05
TORUS = ("za", "zb", "xl", "c", "xh", "y")
SUBCUBE = ("xl", "c", "xh")
SPREAD = ("c", "zb", "za", "xl")
VMEM = pl.BlockSpec(memory_space=pltpu.VMEM)
SMEM = pl.BlockSpec(memory_space=pltpu.SMEM)
F32, BF16 = jnp.float32, jnp.bfloat16


def torus_mesh(mesh):
    groups, parts = mesh.devices.shape
    return Mesh(mesh.devices.reshape(groups // 16, 4, 2, 2, 2, parts // 2), TORUS)


def crossing():
    return [
        ((xl * 2 + c) * 2 + xh, ((1 - xl) * 2 + c) * 2 + (1 - xh))
        for xl in range(2)
        for c in range(2)
        for xh in range(2)
    ]


def gather_y(piece):
    ring = lax.axis_size("y")

    def send(step):
        return lax.ppermute(piece, "y", [(y, (y + step) % ring) for y in range(ring)])

    far = send(2)
    near = send(1)
    other = send(-1)
    return [piece, far, near, other]


def group_index():
    z = lax.axis_index("za") * 4 + lax.axis_index("zb")
    return z * 4 + lax.axis_index("xl") * 2 + lax.axis_index("c")


def order_of(group, groups):
    near = ((group >> 2) & 3) * (groups // 8) + (group >> 4) * 2
    return (group & 1) * (groups // 2) + near + ((group >> 1) & 1)


def pack_kernel(groups, table, rows_in, weights, first, second, leaving, count, rows, staged, sems):
    blocks = rows.shape[0]
    shift = blocks.bit_length() - 1
    quarter = staged.shape[0]
    part = blocks // 4
    xh, core = lax.axis_index("xh"), lax.axis_index("c")
    base = group_index() * blocks
    start = pl.multiple_of(((1 - xh) * 2 + core) * quarter, quarter)
    pieces = [slice(i * part, (i + 1) * part) for i in range(4)]
    loads = [pltpu.make_async_copy(rows_in.at[at], rows.at[at], sems.at[i]) for i, at in enumerate(pieces)]
    load = pltpu.make_async_copy(weights.at[pl.ds(start, quarter), :], staged, sems.at[4])
    store = pltpu.make_async_copy(staged, leaving, sems.at[5])
    for copy in loads:
        copy.start()
    load.start()

    def clear(i, carry):
        count[i] = 0
        return carry

    def put(b, carry):
        target = table[base + b] >> shift
        seen = count[target]
        count[target] = seen + 1
        spot = order_of(target, groups)

        @pl.when(seen == 0)
        def _():
            pltpu.make_async_copy(rows.at[b], first.at[spot], sems.at[6]).start()

        @pl.when(seen != 0)
        def _():
            pltpu.make_async_copy(rows.at[b], second.at[spot], sems.at[7]).start()

        return carry

    lax.fori_loop(0, groups, clear, 0, unroll=8)
    for i in range(4):
        loads[i].wait()
        lax.fori_loop(i * part, (i + 1) * part, put, 0, unroll=4)
        if i == 2:
            load.wait()
            store.start()
    pltpu.make_async_copy(rows.at[0:groups], first, sems.at[6]).wait()
    pltpu.make_async_copy(rows.at[0:groups], second, sems.at[7]).wait()
    store.wait()


def grant(mib):
    return pltpu.CompilerParams(vmem_limit_bytes=mib << 20)


def cost():
    return pl.CostEstimate(flops=1 << 34, bytes_accessed=0, transcendentals=0)


ANY = pl.BlockSpec(memory_space=pl.ANY)


def pack(memory_rows, owner_table, key_weight, groups):
    rows, cols = memory_rows.shape
    width, outs = key_weight.shape
    blocks = rows // BLK
    out = jax.ShapeDtypeStruct((groups, BLK, cols), BF16)
    return pl.pallas_call(
        functools.partial(pack_kernel, groups),
        out_shape=(out, out, jax.ShapeDtypeStruct((width // 4, outs), BF16)),
        in_specs=[SMEM, ANY, ANY],
        out_specs=(ANY, ANY, ANY),
        scratch_shapes=[
            pltpu.SMEM((groups,), jnp.int32),
            pltpu.VMEM((blocks, BLK, cols), BF16),
            pltpu.VMEM((width // 4, outs), BF16),
            pltpu.SemaphoreType.DMA((8,)),
        ],
        cost_estimate=cost(),
        name="pack",
    )(owner_table, memory_rows.reshape(blocks, BLK, cols), key_weight)


def owners():
    y, ring = lax.axis_index("y"), lax.axis_size("y")
    return [y, lax.rem(y + 2, ring), lax.rem(y + ring - 1, ring), lax.rem(y + 1, ring)]


def gain_rows(gain):
    high = gain.astype(BF16).astype(F32)
    middle = (gain - high).astype(BF16).astype(F32)
    zeros = jnp.zeros((BLK - 3, gain.shape[1]), F32)
    return jnp.concatenate([high, middle, gain - high - middle, zeros], axis=0).astype(BF16)


def two_parts(value):
    high = value.astype(BF16).astype(F32)
    return high, value - high


def fold(value):
    lanes = [value[:, i : i + 128] for i in range(0, value.shape[1], 128)]
    return functools.reduce(jnp.add, lanes)


def sent_kernel(p0, p1, p2, p3, gains, w_mine, w_twin, table, sent, raw, scaled, held, sums, acc, sems):
    rows, width = p0.shape
    half = width * 4
    tile = 128
    tiles = rows // BLK
    xh, core = lax.axis_index("xh"), lax.axis_index("c")
    gain = [gains[xh * 4 + owner] for owner in owners()]
    piece_copies = [
        pltpu.make_async_copy(part, raw.at[j], sems.at[j]) for j, part in enumerate((p0, p1, p2, p3))
    ]
    deep = held.shape[0] // 2
    mine_copy = pltpu.make_async_copy(w_mine, held.at[0:deep], sems.at[4])
    twin_copy = pltpu.make_async_copy(w_twin, held.at[deep : 2 * deep], sems.at[5])
    for copy in piece_copies:
        copy.start()
    mine_copy.start()
    twin_copy.start()

    sent[tiles] = jnp.zeros(sent.shape[1:], BF16)
    for j in range(4):
        piece_copies[j].wait()
        for q in range(rows // tile):
            here = pl.ds(q * tile, tile)
            v = raw[j, here, :].astype(F32)
            total, square = fold(v), fold(v * v)
            if j == 0:
                sums[0, here], sums[1, here] = total, square
            else:
                sums[0, here] += total
                sums[1, here] += square
    for q in range(rows // tile):
        here = pl.ds(q * tile, tile)
        mean = jnp.sum(sums[0, here], axis=1, keepdims=True) / half
        square = jnp.sum(sums[1, here], axis=1, keepdims=True) / half
        center, rest = two_parts(mean)
        high, low = two_parts(square - mean * mean)
        for j in range(4):
            v = raw[j, here, :].astype(F32)
            scaled[j, here, :] = ((v - center) * gain[j]).astype(BF16)
        lane = lax.broadcasted_iota(jnp.int32, (tile, 128), 1)
        stats = jnp.where(lane == 0, center, 0.0)
        stats = jnp.where(lane == 1, rest, stats)
        stats = jnp.where(lane == 2, high, stats)
        stats = jnp.where(lane == 3, low, stats)
        table[here, :] = stats
        sent[tiles, :, q * 128 : (q + 1) * 128] = jnp.transpose(stats)[0:BLK, :].astype(BF16)

    mine_copy.wait()
    twin_copy.wait()
    gain_sum = jnp.zeros((BLK, acc.shape[1]), F32)
    for j, owner in enumerate(owners()):
        slot = ((owner >> 1) ^ core) * 2 + (owner & 1)
        block = held[pl.ds(pl.multiple_of(slot * width, width), width), :]
        gain_sum += jnp.dot(gain_rows(gain[j]), block, preferred_element_type=F32)
        part = jnp.dot(scaled[j], block, preferred_element_type=F32)
        if j == 0:
            acc[...] = part
        elif j < 3:
            acc[...] += part
        else:
            sent[0:tiles] = (acc[...] + part).reshape(tiles, BLK, part.shape[1]).astype(BF16)
    total = jnp.sum(gain_sum, axis=0, keepdims=True)
    high, rest = two_parts(total)
    middle, low = two_parts(rest)
    row = lax.broadcasted_iota(jnp.int32, (BLK, width), 0)
    extra = sent[tiles].astype(F32)
    for place, value in ((4, high), (5, middle), (6, low)):
        extra = jnp.where(row == place, value, extra)
    sent[tiles] = extra.astype(BF16)


def project_sent(pieces, gains, mine, twin):
    rows, width = pieces[0].shape
    tiles = rows // BLK
    deep, cols = mine.shape
    return pl.pallas_call(
        sent_kernel,
        out_shape=(
            jax.ShapeDtypeStruct((rows, 128), F32),
            jax.ShapeDtypeStruct((tiles + 1, BLK, cols), BF16),
        ),
        in_specs=[ANY] * 4 + [VMEM] + [ANY] * 2,
        out_specs=(VMEM, VMEM),
        scratch_shapes=[
            pltpu.VMEM((4, rows, width), BF16),
            pltpu.VMEM((4, rows, width), BF16),
            pltpu.VMEM((2 * deep, cols), BF16),
            pltpu.VMEM((2, rows, 128), F32),
            pltpu.VMEM((rows, cols), F32),
            pltpu.SemaphoreType.DMA((6,)),
        ],
        compiler_params=grant(12),
        cost_estimate=cost(),
    )(*pieces, gains, mine, twin)


def kept_kernel(half_id, p0, p1, p2, p3, table, gains, w_own, kept, gain_sums):
    width = p0.shape[1]
    center = table[:, 0:1]
    xh = lax.axis_index("xh")
    total = jnp.zeros((BLK, kept.shape[1]), F32)
    for j, (part, owner) in enumerate(zip((p0, p1, p2, p3), owners())):
        gain = gains[xh * 4 + owner]
        block = w_own[pl.ds(pl.multiple_of(owner * width, width), width), :]
        scaled = ((part[...].astype(F32) - center) * gain).astype(BF16)
        total += jnp.dot(gain_rows(gain), block, preferred_element_type=F32)
        product = jnp.dot(scaled, block, preferred_element_type=F32)
        if j == 0:
            kept[...] = product
        else:
            kept[...] += product
    gain_sums[...] = jnp.broadcast_to(jnp.sum(total, axis=0, keepdims=True), total.shape)


def project_kept(pieces, table, half_id, gains, key_weight):
    rows, width = pieces[0].shape
    half, cols = key_weight.shape[0] // 2, key_weight.shape[1]
    whole = pl.BlockSpec((rows, width), lambda i, s: (0, 0))
    return pl.pallas_call(
        kept_kernel,
        out_shape=(
            jax.ShapeDtypeStruct((rows, cols), F32),
            jax.ShapeDtypeStruct((BLK, cols), F32),
        ),
        grid_spec=pltpu.PrefetchScalarGridSpec(
            num_scalar_prefetch=1,
            grid=(1,),
            in_specs=[whole] * 4
            + [
                pl.BlockSpec((rows, 128), lambda i, s: (0, 0)),
                pl.BlockSpec(gains.shape, lambda i, s: (0, 0, 0)),
                pl.BlockSpec((half, cols), lambda i, s: (s[0], 0)),
            ],
            out_specs=(
                pl.BlockSpec((rows, cols), lambda i, s: (0, 0)),
                pl.BlockSpec((BLK, cols), lambda i, s: (0, 0)),
            ),
        ),
        compiler_params=grant(16),
        cost_estimate=cost(),
    )(half_id, *pieces, table, gains, key_weight)


def whole_keys(kept, table, came, gain_sums, q):
    tiles = came.shape[0] - 1
    cols = came.shape[2]
    here = pl.ds(q * 128, 128)
    per = 128 // BLK
    value_b = came[q * per : (q + 1) * per].astype(F32).reshape(128, cols)
    stats = came[tiles, :, q * 128 : (q + 1) * 128].astype(F32)
    stats = jnp.concatenate([stats, jnp.zeros((128 - BLK, 128), F32)], axis=0)
    stats_b = jnp.transpose(stats)
    stats_a = table[here, :]
    center_a, center_b = stats_a[:, 0:1], stats_b[:, 0:1]
    mean_a, mean_b = center_a + stats_a[:, 1:2], center_b + stats_b[:, 1:2]
    var_a, var_b = stats_a[:, 2:3] + stats_a[:, 3:4], stats_b[:, 2:3] + stats_b[:, 3:4]
    mean = 0.5 * (mean_a + mean_b)
    gap = 0.5 * (mean_a - mean_b)
    scale = lax.rsqrt(0.5 * (var_a + var_b) + gap * gap + EPS)
    sums_b = jnp.sum(came[tiles, 4:7, :].astype(F32), axis=0, keepdims=True)
    shift = (center_a - mean) * gain_sums[0:1, :] + (center_b - mean) * sums_b
    keys = (kept[here, :] + value_b + shift) * scale
    return keys.reshape(per, BLK, cols).astype(BF16)


def sum_kernel(kept, table, came, gain_sums, out):
    per = 128 // BLK
    for q in range(kept.shape[0] // 128):
        out[q * per : (q + 1) * per] = whole_keys(kept, table, came, gain_sums, q)


def sum_partials(kept, table, came, gain_sums):
    tiles, _, cols = came.shape
    return pl.pallas_call(
        sum_kernel,
        out_shape=jax.ShapeDtypeStruct((tiles - 1, BLK, cols), BF16),
        in_specs=[VMEM] * 4,
        out_specs=VMEM,
        compiler_params=grant(16),
        cost_estimate=cost(),
        name="sum_g",
    )(kept, table, came, gain_sums)


def place_kernel(slots, kept, table, came, gain_sums, others, out):
    groups = others.shape[0]
    per = 128 // BLK
    for q in range(kept.shape[0] // 128):
        keys = whole_keys(kept, table, came, gain_sums, q)
        for i in range(per):
            out[slots[q * per + i]] = keys[i]

    def put(i, carry):
        out[slots[groups + i]] = others[i]
        return carry

    lax.fori_loop(0, groups, put, 0, unroll=8)


def place(slots, kept, table, came, gain_sums, others):
    _, _, cols = came.shape
    blocks = slots.shape[0]
    return pl.pallas_call(
        place_kernel,
        out_shape=jax.ShapeDtypeStruct((blocks, BLK, cols), BF16),
        in_specs=[SMEM] + [VMEM] * 5,
        out_specs=VMEM,
        compiler_params=grant(16),
        cost_estimate=cost(),
        name="place",
    )(slots, kept, table, came, gain_sums, others)


def arrival_slots(owner_table, group, groups, blocks):
    table = owner_table.reshape(groups, blocks)
    ids = jnp.arange(blocks, dtype=jnp.int32)[None, :]
    here = table // blocks == group
    first = jnp.min(jnp.where(here, ids, blocks), axis=1, keepdims=True)
    slots = table % blocks
    slot_a = jnp.sum(jnp.where(ids == first, slots, 0), axis=1)
    slot_b = jnp.sum(jnp.where(here & (ids != first), slots, 0), axis=1)
    by_source = [
        slot.reshape(groups // 16, 4, 2, 2).transpose(3, 1, 0, 2).reshape(groups) for slot in (slot_a, slot_b)
    ]
    return jnp.concatenate(by_source)


def steps(memory_rows, norm_gain, key_weight, owner_table):
    groups = owner_table.shape[0] // (memory_rows.shape[0] // BLK)
    xh, group = lax.axis_index("xh"), group_index()
    rows, cols = memory_rows.shape
    blocks, half_rows = rows // BLK, rows // 2
    width, outs = key_weight.shape

    packed_p, packed_g, leaving = pack(memory_rows, owner_table, key_weight, groups)
    mine = lax.ppermute(leaving, SUBCUBE, crossing())
    twin = lax.ppermute(mine, "c", [(0, 1), (1, 0)])
    pieces_g = gather_y(packed_g.reshape(half_rows, cols))
    rows_p = lax.all_to_all(packed_p, SPREAD, 0, 0, tiled=True)

    gains = norm_gain.reshape(width // cols, 1, cols)
    half_id = xh.reshape(1).astype(jnp.int32)
    slots = arrival_slots(owner_table, group, groups, blocks)

    pair = [(0, 1), (1, 0)]
    table_g, sent_g = project_sent(pieces_g, gains, mine, twin)
    came_g = lax.ppermute(sent_g, "xh", pair)
    kept_g, gain_sums_g = project_kept(pieces_g, table_g, half_id, gains, key_weight)
    keys_g = sum_partials(kept_g, table_g, came_g, gain_sums_g)
    keys_g = lax.all_to_all(keys_g, SPREAD, 0, 0, tiled=True)

    pieces_p = gather_y(rows_p.reshape(half_rows, cols))
    table_p, sent_p = project_sent(pieces_p, gains, mine, twin)
    came_p = lax.ppermute(sent_p, "xh", pair)
    kept_p, gain_sums_p = project_kept(pieces_p, table_p, half_id, gains, key_weight)
    placed = place(slots, kept_p, table_p, came_p, gain_sums_p, keys_g)
    return placed.reshape(rows, outs)


def solution(mesh):
    groups, parts = ("za", "zb", "xl", "c"), ("xh", "y")
    torus = torus_mesh(mesh)
    return jax.shard_map(
        steps,
        mesh=torus,
        in_specs=(P(groups, parts), P(), P(None, parts), P()),
        out_specs=P(groups, parts),
        check_vma=False,
    )
```
